32 devices in a mesh: layer: 4 (over y, core), col: 4 (over z), row: 2 (over x).
Axes of the slice: x: 2, y: 2, z: 4, core: 2. Of those that a mesh axis runs over, the one named last changes fastest.
Arguments:
- activations: bfloat16 [4, 768, 4096], P(None, ('layer', 'row'), 'col'), may hold values from -6 to 6
- out_grads: bfloat16 [4, 768, 11008], P(None, ('layer', 'col'), 'row'), may hold values from -0.02734375 to 0.02734375
- basis_in: bfloat16 [4, 4096, 4096], P('layer', 'col', 'row'), may hold values from -0.09375 to 0.09375
- basis_out: bfloat16 [4, 11008, 11008], P('layer', 'row', 'col'), may hold values from -0.0546875 to 0.0546875
- eigenvalues: float32 [4, 11008, 4096], P('layer', 'col', 'row'), may hold values from 0.01 to 10
- damping: float32 [4], P('layer'), may hold values from 0.05 to 0.5
- layer_order: int32 [4], replicated, may hold values from 0 to 3, each once
- query_ids: int32 [256], replicated, may hold values from 0 to 3, never falling along the last dimension, each value on 1 to 128 neighbouring positions
- train_ids: int32 [512], replicated, may hold values from 0 to 15, never falling along the last dimension, each value on 1 to 64 neighbouring positions
Outputs:
- scores: float32 [4, 16], replicated
The draws below stay inside these ranges and needn't reach their ends.
Inputs may be any that keep to these rules, and one draw needn't show every extreme that they name: `layer_order`: each slot's layer appears once. `query_ids`: never falling; every query example has 1 to 128 tokens. `train_ids`: never falling; every train example has 1 to 64 tokens.
All inputs are finite; a program needn't handle non-finite values.
Results may differ from the reference program's by a relative error of at most 0.02.
Values may be sent and summed in bfloat16 or wider, within the bound.
No kernel may reach another device: no remote copies, remote signals or barrier semaphores. Data moves between devices by JAX's collectives and lax.ppermute only.
A program may use at most 192 MiB of HBM per device.

```python
import math
import jax
import jax.numpy as jnp
import numpy as np
from jax import lax

DIN = 4096
DOUT = 11008
LAYERS = 4
QUERIES = 4
TRAIN = 16
QLEN = 64
TLEN = 32
QTOK = 256
TTOK = 512
QMOST = 128
TMOST = 64
N_COL = 4
N_ROW = 2


def level_of(stream_key, shape, cuts, least, top_value):
    gain = 1.0
    for position, parts in cuts:
        draws = jax.random.uniform(jax.random.fold_in(jax.random.fold_in(stream_key, 6), position), (parts,), jnp.float32, least / len(cuts), top_value / len(cuts))
        gain = gain * jnp.repeat(jnp.exp(draws), shape[position] // parts).reshape((-1,) + (1,) * (len(shape) - 1 - position))
    return gain


def length_profile(number_of, total, bound, lean):
    weights = [(1 << 20) // math.isqrt(standing ** lean) + 1 for standing in range(2, number_of + 1)]
    rest, holding = total - bound - (number_of - 1), [1] * (number_of - 1)
    while rest > 0:
        free = [i for i in range(number_of - 1) if holding[i] < bound]
        mass, remaining = sum([weights[i] for i in free]), rest
        for i in free:
            addition = min(bound - holding[i], max(1, remaining * weights[i] // mass), rest)
            holding[i] = holding[i] + addition
            rest = rest - addition
    return np.array([bound] + holding)


def ragged_sizes(rng, amount, total, most, skew):
    if amount == 2:
        one = jax.random.randint(rng, (), max(1, total - most), min(most, total - 1) + 1)
        return jnp.stack([one, total - one])
    lengths = jnp.asarray(length_profile(amount, total, most, skew), jnp.int32)
    twos = (amount - 1) // 2
    giver, receiver = lengths[1:1 + 2 * twos:2], lengths[2:2 + 2 * twos:2]
    room = jnp.minimum(giver - 1, most - receiver)
    moved = jax.random.randint(jax.random.fold_in(rng, 1), (twos,), 0, 1 << 20) % (room + 1)
    lengths = lengths.at[1:1 + 2 * twos:2].set(giver - moved).at[2:2 + 2 * twos:2].set(receiver + moved)
    return lengths[jax.random.permutation(jax.random.fold_in(rng, 2), amount)]


def normal_values(stream_key, extent, spread, reach, pieces=(), kind=jnp.bfloat16):
    array = spread * jax.random.normal(stream_key, extent, jnp.float32)
    if pieces:
        array = array * level_of(stream_key, extent, pieces, -0.22, 0.18)
    return jnp.clip(array, -reach, reach).astype(kind)


def setup_inputs(seed: int = 0) -> dict:
    streams_of = jax.random.split(jax.random.key(seed), 10)
    activations = normal_values(streams_of[0], (LAYERS, QTOK + TTOK, DIN), 1.0, 6.0, ((1, 8), (2, 4)))
    out_grads = normal_values(streams_of[1], (LAYERS, QTOK + TTOK, DOUT), ((QLEN * TLEN * DIN * DOUT) ** -0.25), 0.02734375, ((1, 16), (2, 2)))
    basis_in = normal_values(streams_of[2], (LAYERS, DIN, DIN), DIN ** -0.5, 0.09375, ((0, 4), (1, 4), (2, 2)))
    basis_out = normal_values(streams_of[3], (LAYERS, DOUT, DOUT), DOUT ** -0.5, 0.0546875, ((0, 4), (1, 2), (2, 4)))
    eigenvalues = jnp.clip(jnp.exp(math.log(10.0) - 6.9077553 * jax.random.uniform(streams_of[4], (LAYERS, DOUT, DIN), jnp.float32) ** level_of(streams_of[4], (LAYERS, DOUT, DIN), ((0, 4), (1, 4), (2, 2)), -0.2, 0.2)), 0.01, 10.0)
    damping = jnp.clip(jnp.exp(math.log(0.5) - 2.3025851 * jax.random.uniform(streams_of[5], (LAYERS,), jnp.float32) ** level_of(streams_of[5], (LAYERS,), ((0, 4),), -0.2, 0.2)), 0.05, 0.5)
    layer_order = jax.random.permutation(streams_of[6], LAYERS).astype(jnp.int32)
    query_ids = jnp.searchsorted(jnp.cumsum(ragged_sizes(streams_of[7], QUERIES, QTOK, QMOST, 1)), jnp.arange(QTOK), side="right").astype(jnp.int32)
    train_ids = jnp.searchsorted(jnp.cumsum(ragged_sizes(streams_of[8], TRAIN, TTOK, TMOST, 1)), jnp.arange(TTOK), side="right").astype(jnp.int32)
    return {"activations": activations, "out_grads": out_grads, "basis_in": basis_in, "basis_out": basis_out, "eigenvalues": eigenvalues, "damping": damping, "layer_order": layer_order, "query_ids": query_ids, "train_ids": train_ids}


def rotate(values, basis, blocks):
    width = basis.shape[0] // blocks
    total = jnp.zeros((values.shape[0], basis.shape[1]), jnp.float32)
    for index in range(blocks):
        piece = jnp.dot(values[:, index * width:(index + 1) * width], basis[index * width:(index + 1) * width], preferred_element_type=jnp.float32)
        rounded = lax.optimization_barrier(piece.astype(jnp.bfloat16))
        total = total + rounded.astype(jnp.float32)
    return total.astype(jnp.bfloat16)


def reference(activations, out_grads, basis_in, basis_out, eigenvalues, damping, layer_order, query_ids, train_ids):
    query_tokens = query_ids.shape[0]
    train_onehot = (train_ids[:, None] == jnp.arange(TRAIN, dtype=jnp.int32)[None, :]).astype(jnp.float32)
    total = jnp.zeros((QUERIES, TRAIN), jnp.float32)
    for slot in range(LAYERS):
        layer = layer_order[slot].astype(jnp.int32)
        inputs = lax.dynamic_index_in_dim(activations, layer, 0, keepdims=False)
        grads = lax.dynamic_index_in_dim(out_grads, layer, 0, keepdims=False)
        rotated_in = rotate(inputs, basis_in[slot], N_COL)
        rotated_out = rotate(grads, basis_out[slot], N_ROW)
        query_in = rotated_in[:query_tokens]
        query_out = rotated_out[:query_tokens]
        train_in = rotated_in[query_tokens:]
        train_out = rotated_out[query_tokens:]
        denominator = eigenvalues[slot] + damping[slot]

        def one_query(index):
            mask = (query_ids == index).astype(jnp.bfloat16)
            masked = query_in * mask[:, None]
            gram = jnp.dot(query_out.T, masked, preferred_element_type=jnp.float32)
            precond = (gram / denominator).astype(jnp.bfloat16)
            mapped = jnp.dot(train_out, precond, preferred_element_type=jnp.float32)
            return jnp.sum(mapped * train_in.astype(jnp.float32), axis=1)

        values = lax.map(one_query, jnp.arange(QUERIES, dtype=jnp.int32))
        total = total + jnp.dot(values, train_onehot, precision=lax.Precision.HIGHEST)
    return total
```

```python
import jax
import jax.numpy as jnp
from jax import lax
from jax.experimental.layout import Layout, with_layout_constraint
from jax.sharding import PartitionSpec as P


QUERIES = 4
TRAIN = 16
F32 = jnp.float32
BF16 = jnp.bfloat16


def exchange_sum(x, axis):
    size = lax.axis_size(axis)
    step = 1
    while step < size:
        x = x + lax.ppermute(x, axis, [(i, i ^ step) for i in range(size)])
        step *= 2
    return x


def body(
    activations,
    out_grads,
    basis_in,
    basis_out,
    eigenvalues,
    damping,
    layer_order,
    query_ids,
    train_ids,
):
    groups = lax.axis_size("layer")
    rows = lax.axis_size("row")
    cols = lax.axis_size("col")
    g = lax.axis_index("layer")
    r = lax.axis_index("row")
    c = lax.axis_index("col")
    out_tokens = out_grads.shape[1]
    block = out_tokens * cols
    tokens = block * groups
    query_tokens = query_ids.shape[0]
    rest = 2 * block - query_tokens
    odd = g % 2
    low = g < groups // 2

    place = jnp.arange(groups, dtype=jnp.int32)
    wanted = jnp.sum(jnp.where((g ^ place)[:, None] == place[None, :], layer_order[None, :], 0), axis=1)

    def moved(x, m):
        if m == 0:
            return x[0]
        return lax.ppermute(x[m], "layer", [(i, i ^ m) for i in range(groups)])

    def ring_pieces(piece, axis):
        size = lax.axis_size(axis)
        ring = [(i, (i + 1) % size) for i in range(size)]
        pieces = [piece]
        for _ in range(1, size):
            pieces.append(lax.ppermute(pieces[-1], axis, ring))
        return pieces

    sent_out = jnp.take(out_grads, wanted, axis=0, mode="clip")
    sent_in = jnp.take(activations, wanted, axis=0, mode="clip")
    got_out = [moved(sent_out, m) for m in range(groups)]
    got_in = [moved(sent_in, m) for m in range(groups)]

    early = 2 + odd
    pieces = []
    for m in range(groups):
        pieces += ring_pieces(got_in[m], "row")
    source_layer = jnp.where(place < 2, place, jnp.where(place == 2, early, 5 - early))
    step = (r - jnp.arange(rows, dtype=jnp.int32)) % rows
    index = ((source_layer ^ g)[:, None] * rows + step[None, :]).reshape(-1)
    stacked = jnp.stack(pieces)
    inputs_full = jnp.take(stacked, index, axis=0, mode="clip").reshape(tokens, activations.shape[2])
    partial_in = jnp.dot(inputs_full, basis_in[0], preferred_element_type=F32).astype(BF16)

    size = query_tokens

    def summed(k):
        own = lax.optimization_barrier(partial_in[k * size : (k + 1) * size])
        total = own.astype(F32)
        got = None
        for t in range(cols - 1):
            sent = own if got is None else (own.astype(F32) + got.astype(F32)).astype(BF16)
            got = lax.ppermute(sent, "col", [(t, t + 1), (cols - 1 - t, cols - 2 - t)])
            total = total + got.astype(F32)
        return total.astype(BF16)

    slices = [summed(k) for k in range(tokens // size)]

    first_late, last_late = lax.optimization_barrier(
        (jnp.where(low, got_out[1], got_out[3]), jnp.where(low, got_out[3], got_out[1]))
    )

    def gathered(piece):
        parts = ring_pieces(piece, "col")
        placed = []
        for k in range(cols):
            part = parts[-k % cols]
            for at in range(1, cols):
                part = jnp.where(c == at, parts[(at - k) % cols], part)
            placed.append(part)
        return lax.optimization_barrier(jnp.concatenate(placed))

    def rotated(full):
        own = jnp.dot(full, basis_out[0], preferred_element_type=F32).astype(BF16)
        step = 1
        while step < rows:
            got = lax.ppermute(own, "row", [(i, i ^ step) for i in range(rows)])
            own = (own.astype(F32) + got.astype(F32)).astype(BF16)
            step *= 2
        return own

    wide = [gathered(piece) for piece in (got_out[0], got_out[2], first_late, last_late)]
    mine, paired, third, last = [rotated(full) for full in wide]
    known = jnp.where(low, mine, paired)
    other = jnp.where(low, paired, mine)
    even = odd == 0
    zero = jnp.where(even, known, third)
    one = jnp.where(even, third, known)
    query_out, rest_out, other = lax.optimization_barrier(
        (jnp.concatenate([zero, one[: block - rest]]), one[block - rest :], other)
    )
    train_out = jnp.concatenate([rest_out, other, last])

    denominator = lax.optimization_barrier(eigenvalues[0] + damping[0])
    query_in = slices[0]
    query_mask = (query_ids[None, :] == jnp.arange(QUERIES, dtype=jnp.int32)[:, None]).astype(BF16)
    masked = query_mask[:, :, None] * query_in[None, :, :]
    gram = jnp.einsum("si,qsj->qij", query_out, masked, preferred_element_type=F32)
    precond = lax.optimization_barrier((gram / denominator).astype(BF16))
    mapped = jnp.einsum("ui,qij->qju", train_out, precond, preferred_element_type=F32).astype(BF16)
    mapped = lax.optimization_barrier(mapped)
    values = []
    for k in range(1, tokens // size):
        part = with_layout_constraint(slices[k].T, Layout((0, 1)))
        part = lax.optimization_barrier(part).astype(F32)
        values.append(jnp.sum(mapped[:, :, (k - 1) * size : k * size].astype(F32) * part[None], axis=1))
    values = jnp.concatenate(values, axis=1)

    train_onehot = (train_ids[:, None] == jnp.arange(TRAIN, dtype=jnp.int32)[None, :]).astype(F32)
    onehot = jnp.concatenate(
        [
            train_onehot[:rest],
            lax.dynamic_slice_in_dim(train_onehot, early * block - query_tokens, block),
            lax.dynamic_slice_in_dim(train_onehot, (5 - early) * block - query_tokens, block),
        ]
    )
    total = jnp.dot(values, onehot, precision=lax.Precision.HIGHEST)
    for axis in ("row", "layer", "col"):
        total = exchange_sum(total, axis)
    return total


def solution(mesh):
    in_specs = (
        P(None, ("layer", "row"), "col"),
        P(None, ("layer", "col"), "row"),
        P("layer", "col", "row"),
        P("layer", "row", "col"),
        P("layer", "col", "row"),
        P("layer"),
        P(),
        P(),
        P(),
    )
    out_specs = P()
    return jax.shard_map(body, mesh=mesh, in_specs=in_specs, out_specs=out_specs, check_vma=False)
```
